32 devices in a mesh: dp: 4 (over y, core), lat: 4 (over z), chan: 2 (over x).
Axes of the slice: x: 2, y: 2, z: 4, core: 2. Of those that a mesh axis runs over, the one named last changes fastest.
Arguments:
- saved_input: bfloat16 [4, 16, 720, 1024], P('dp', None, 'lat', 'chan'), may hold values from -6 to 6
- grad_output: bfloat16 [4, 16, 720, 1024], P('dp', None, 'lat', 'chan'), may hold values from -6 to 6
- legendre: bfloat16 [16, 192, 720], P('lat'), may hold values from -0.21875 to 0.21875
- quad_weight: float32 [720], replicated, may hold values from 0.3 to 3
- mixing_weight: bfloat16 [192, 512, 1024], P('lat', None, 'chan'), may hold values from -0.375 to 0.375
Outputs:
- grad_weight: bfloat16 [192, 512, 1024], P('lat', 'dp', 'chan')
- grad_input: bfloat16 [4, 16, 720, 1024], P('dp', None, 'lat', 'chan')
The draws below stay inside these ranges and needn't reach their ends.
All inputs are finite; a program needn't handle non-finite values.
Results may differ from the reference program's by a relative error of at most 0.014.
Values may be sent and summed in bfloat16 or wider, within the bound.
No kernel may reach another device: no remote copies, remote signals or barrier semaphores. Data moves between devices by JAX's collectives and lax.ppermute only.
A program may use at most 192 MiB of HBM per device.

```python
import math
import jax
import jax.numpy as jnp
from jax import lax

NLAT = 720
L = 192
C = 512
BATCH = 4
M = 16
N_DP = 4
N_CHAN = 2


def strengthened(result, rng, source, target, blocks, factor):
    def block_of(axis_at):
        return (jnp.arange(result.shape[axis_at]) // (result.shape[axis_at] // blocks)).reshape((-1,) + (1,) * (result.ndim - 1 - axis_at))

    first = jax.random.permutation(rng, blocks)[block_of(target)]
    other_side = (block_of(target) + blocks // 2) % blocks
    return jnp.where((block_of(source) == first) | (block_of(source) == other_side), factor * result, result)


def level_of(rng, extent, split, low, top_value):
    def one(axis_at, blocks):
        draws = jax.random.uniform(jax.random.fold_in(jax.random.fold_in(rng, 6), axis_at), (blocks,), jnp.float32, low / len(split), top_value / len(split))
        return jnp.repeat(jnp.exp(draws), extent[axis_at] // blocks).reshape((-1,) + (1,) * (len(extent) - axis_at - 1))

    gain = one(*split[0])
    for cut in split[1:]:
        gain = gain * one(*cut)
    return gain


def gaussian(key, shape, scale, limit, shards=(), held_as=jnp.bfloat16):
    factor_of = level_of(key, shape, shards, -0.22, 0.18) if shards else 1.0
    values = jax.random.normal(key, shape, jnp.float32) * scale * factor_of
    return jnp.minimum(jnp.maximum(values, -limit), limit).astype(held_as)


def bell_draw_with(stream_key, extent, deviation, limit, split, heavy, dtype=jnp.bfloat16):
    values = deviation * jax.random.normal(stream_key, extent, jnp.float32)
    if split:
        values = values * level_of(stream_key, extent, split, -0.22, 0.18)
    return jnp.clip(strengthened(values, jax.random.fold_in(stream_key, 3), *heavy), -limit, limit).astype(dtype)


def setup_inputs(seed: int = 0) -> dict:
    key_list = jax.random.split(jax.random.key(seed), 6)
    saved_input = bell_draw_with(key_list[0], (BATCH, M, NLAT, 2 * C), 1.0, 6.0, ((0, 4), (2, 4), (3, 2)), (0, 3, 4, 2.0))
    grad_output = gaussian(key_list[1], (BATCH, M, NLAT, 2 * C), 1.0, 6.0, ((0, 4), (2, 4), (3, 2)))
    legendre = gaussian(key_list[2], (M, L, NLAT), NLAT ** -0.5, 0.21875, ((0, 4),))
    quad_weight = jnp.clip(jnp.exp(jax.random.uniform(key_list[3], (NLAT,), jnp.float32, math.log(0.3), math.log(3.0))), 0.3, 3.0)
    mixing_weight = bell_draw_with(key_list[4], (L, C, 2 * C), C ** -0.5, 0.375, ((0, 4), (2, 2)), (2, 1, 2, 2.0))
    return {"saved_input": saved_input, "grad_output": grad_output, "legendre": legendre, "quad_weight": quad_weight, "mixing_weight": mixing_weight}


def partner_of(grads):
    pairs = grads.reshape(grads.shape[:-1] + (grads.shape[-1] // 2, 2))
    swapped = jnp.stack([pairs[..., 1], -pairs[..., 0]], axis=-1)
    return swapped.reshape(grads.shape)


def weight_terms(spectra, grads):
    pairs = spectra.reshape(spectra.shape[:-1] + (spectra.shape[-1] // 2, 2))
    partner = partner_of(grads)
    first = jnp.einsum('bmli,bmlq->liq', pairs[..., 0], grads)
    second = jnp.einsum('bmli,bmlq->liq', pairs[..., 1], partner)
    return first + second


def reference(saved_input, grad_output, legendre, quad_weight, mixing_weight):
    analysis = (legendre.astype(jnp.float32) * quad_weight[None, None, :]).astype(jnp.bfloat16)
    analysis_wide = analysis.astype(jnp.float32)
    spectra = jnp.einsum('mlj,bmjq->bmlq', analysis_wide, saved_input.astype(jnp.float32)).astype(jnp.bfloat16)
    grad_spectra = jnp.einsum('mlj,bmjq->bmlq', legendre.astype(jnp.float32), grad_output.astype(jnp.float32)).astype(jnp.bfloat16)
    batch = saved_input.shape[0]
    spec_wide = spectra.astype(jnp.float32)
    grad_wide = grad_spectra.astype(jnp.float32)
    spec_groups = spec_wide.reshape((N_DP, batch // N_DP) + spec_wide.shape[1:])
    grad_groups = grad_wide.reshape((N_DP, batch // N_DP) + grad_wide.shape[1:])

    def add_group(running, members):
        term = weight_terms(members[0], members[1]) / batch
        rounded = lax.optimization_barrier(term.astype(jnp.bfloat16))
        return running + rounded.astype(jnp.float32), None

    initial = jnp.zeros(mixing_weight.shape, jnp.float32)
    summed, unused = lax.scan(add_group, initial, (spec_groups, grad_groups))
    grad_weight = summed.astype(jnp.bfloat16)

    width = 2 * C // N_CHAN
    partner_wide = partner_of(grad_wide)
    grad_blocks = jnp.moveaxis(grad_wide.reshape(grad_wide.shape[:3] + (N_CHAN, width)), 3, 0)
    partner_blocks = jnp.moveaxis(partner_wide.reshape(partner_wide.shape[:3] + (N_CHAN, width)), 3, 0)
    weight_wide = mixing_weight.astype(jnp.float32)
    weight_blocks = jnp.moveaxis(weight_wide.reshape(weight_wide.shape[:2] + (N_CHAN, width)), 2, 0)

    def add_block(running, members):
        grads_block, partner_block, weights_block = members
        sum_real = jnp.einsum('bmlq,liq->bmli', grads_block, weights_block)
        sum_imag = jnp.einsum('bmlq,liq->bmli', partner_block, weights_block)
        term = jnp.stack([sum_real, sum_imag], axis=-1).reshape(running.shape)
        rounded = lax.optimization_barrier(term.astype(jnp.bfloat16))
        return running + rounded.astype(jnp.float32), None

    start_sum = jnp.zeros(spec_wide.shape, jnp.float32)
    spec_sum, unused_two = lax.scan(add_block, start_sum, (grad_blocks, partner_blocks, weight_blocks))
    grad_spec_in = spec_sum.astype(jnp.bfloat16)
    grad_input = jnp.einsum('mlj,bmlq->bmjq', analysis_wide, grad_spec_in.astype(jnp.float32)).astype(jnp.bfloat16)
    return (grad_weight, grad_input)
```

```python
import functools

import jax
import jax.numpy as jnp
from jax import lax
from jax.experimental import pallas as pl
from jax.experimental.pallas import tpu as pltpu
from jax.sharding import PartitionSpec as P

HALVES = 2
BF16, F32 = jnp.bfloat16, jnp.float32


def swap_pairs(n, bit):
    return [(i, i ^ bit) for i in range(n)]


def partner_rows(rows):
    wide = rows.astype(F32)
    axis = rows.ndim - 1
    width = rows.shape[-1]
    even = lax.broadcasted_iota(jnp.int32, rows.shape, axis) % 2 == 0
    following = pltpu.roll(wide, width - 1, axis)
    preceding = pltpu.roll(wide, 1, axis)
    return jnp.where(even, following, -preceding).astype(rows.dtype)


def mix_body(half_ref, grads_ref, weight_ref, out_ref):
    del half_ref
    for l in range(grads_ref.shape[0]):
        grads = grads_ref[l]
        rows = jnp.concatenate([grads, partner_rows(grads)], axis=0)
        sums = lax.dot_general(
            rows, weight_ref[l], (((1,), (1,)), ((), ())), preferred_element_type=F32
        )
        m, width = grads.shape[0], weight_ref.shape[1]
        out_ref[l, :, :width] = sums[:m].astype(out_ref.dtype)
        out_ref[l, :, width:] = sums[m:].astype(out_ref.dtype)


def mix(grads, weight, block, blocks):
    degrees, orders, width = grads.shape
    rows = weight.shape[1] // blocks
    step = 4 if degrees % 4 == 0 else 1
    return pl.pallas_call(
        mix_body,
        grid_spec=pltpu.PrefetchScalarGridSpec(
            num_scalar_prefetch=1,
            grid=(degrees // step,),
            in_specs=[
                pl.BlockSpec((step, orders, width), lambda l, b: (l, 0, 0)),
                pl.BlockSpec((step, rows, width), lambda l, b: (l, b[0], 0)),
            ],
            out_specs=pl.BlockSpec((step, orders, 2 * rows), lambda l, b: (l, 0, 0)),
        ),
        out_shape=jax.ShapeDtypeStruct((degrees, orders, 2 * rows), BF16),
        cost_estimate=pl.CostEstimate(
            flops=4 * degrees * orders * rows * width,
            bytes_accessed=2 * degrees * rows * width,
            transcendentals=0,
        ),
        name="mix",
    )(block.reshape(1), grads, weight)


def weight_body(scale, count, *refs):
    grads_refs, spectra_refs, out_ref = refs[:count], refs[count : 2 * count], refs[-1]
    for l in range(out_ref.shape[0]):
        grads = jnp.concatenate([ref[l] for ref in grads_refs], axis=0)
        right = jnp.concatenate([grads, partner_rows(grads)], axis=0)
        spectra = jnp.concatenate([ref[l] for ref in spectra_refs], axis=0)
        width = spectra.shape[1] // 2
        left = jnp.concatenate([spectra[:, :width], spectra[:, width:]], axis=0)
        sums = lax.dot_general(left, right, (((0,), (0,)), ((), ())), preferred_element_type=F32)
        out_ref[l] = (sums * scale).astype(out_ref.dtype)


def weight_gradient(grads, spectra, scale):
    degrees, orders, width = grads[0].shape
    rows = spectra[0].shape[2] // 2
    step = 4 if degrees % 4 == 0 else 1
    take = lambda l: (l, 0, 0)
    return pl.pallas_call(
        functools.partial(weight_body, scale, len(grads)),
        grid=(degrees // step,),
        in_specs=[pl.BlockSpec((step, orders, width), take)] * len(grads)
        + [pl.BlockSpec((step, orders, 2 * rows), take)] * len(grads),
        out_specs=pl.BlockSpec((step, rows, width), take),
        out_shape=jax.ShapeDtypeStruct((degrees, rows, width), BF16),
        cost_estimate=pl.CostEstimate(
            flops=4 * len(grads) * degrees * orders * rows * width,
            bytes_accessed=2 * degrees * rows * width,
            transcendentals=0,
        ),
        name="weight_gradient",
    )(*grads, *spectra)


def split_table(legendre, n, z):
    orders, degrees, lats = legendre.shape
    n_dp = lax.axis_size("dp")
    share = 2 if n_dp % 2 == 0 and orders % 2 == 0 else 1
    mine = lax.axis_index("dp") % share
    part = orders // share
    by_lat = legendre.reshape(share, part, degrees, n, lats // n).transpose(3, 0, 1, 2, 4)
    table = jnp.zeros((n, part, degrees, lats // n), legendre.dtype)
    for s in range(n):
        piece = lax.dynamic_slice(
            by_lat, ((z + s) % n, mine, 0, 0, 0), (1, 1) + by_lat.shape[2:]
        ).reshape(by_lat.shape[2:])
        if s:
            piece = lax.ppermute(piece, "lat", [(i, (i + s) % n) for i in range(n)])
        table = lax.dynamic_update_slice(table, piece[None], ((z - s) % n, 0, 0, 0))
    if share == 2:
        other = lax.ppermute(table, "dp", swap_pairs(n_dp, 1))
        first = jnp.where(mine == 0, table, other)
        second = jnp.where(mine == 0, other, table)
        table = jnp.stack([first, second], axis=1)
    table = table.reshape(n * orders, n, degrees // n, lats // n).transpose(1, 0, 2, 3)
    return jnp.concatenate(
        [lax.dynamic_slice_in_dim(table, (z + k) % n, 1, axis=0) for k in range(n)], axis=0
    )


def line(n, count, sign):
    if sign > 0:
        return [(i, i + 1) for i in range(count)]
    return [(n - 1 - i, n - 2 - i) for i in range(count)]


def reduce_scatter_line(parts, n):
    above = below = None
    for r in range(1, n):
        send_up, send_down = parts[n - r], parts[r]
        if r > 1:
            send_up = (send_up.astype(F32) + above.astype(F32)).astype(BF16)
            send_down = (send_down.astype(F32) + below.astype(F32)).astype(BF16)
        above = lax.ppermute(send_up, "lat", line(n, r, 1))
        below = lax.ppermute(send_down, "lat", line(n, r, -1))
    total = parts[0].astype(F32)
    if n > 1:
        total = total + above.astype(F32) + below.astype(F32)
    return total.astype(BF16)


def all_gather_line(block, n):
    ups, downs = [block], [block]
    for r in range(1, n):
        ups.append(lax.ppermute(ups[-1], "lat", [(i, i + 1) for i in range(r - 1, n - 1)]))
        downs.append(lax.ppermute(downs[-1], "lat", [(i + 1, i) for i in range(n - r)]))
    return [block] + [downs[k] + ups[n - k] for k in range(1, n)]


def degree_spectra(table, values, n):
    halves = []
    orders = values.shape[0]
    for h in range(HALVES):
        rows = slice(h * orders // HALVES, (h + 1) * orders // HALVES)
        terms = jnp.einsum(
            "kmlj,mjq->kmlq", table[:, rows], values[rows], preferred_element_type=F32
        ).astype(BF16)
        halves.append(reduce_scatter_line([terms[k] for k in range(n)], n))
    return jnp.concatenate(halves, axis=0)


def on_device(saved_input, grad_output, legendre, quad_weight, mixing_weight):
    n_lat, n_dp, n_chan = (lax.axis_size(a) for a in ("lat", "dp", "chan"))
    z, d, c = (lax.axis_index(a) for a in ("lat", "dp", "chan"))
    samples, orders, lats, width = saved_input.shape
    degrees = mixing_weight.shape[0]
    batch = samples * n_dp

    table = split_table(legendre, n_lat, z)
    quad = lax.dynamic_slice_in_dim(quad_weight, z * lats, lats)
    analysis = (table.astype(F32) * quad).astype(BF16)

    fold = lambda a: a.reshape((samples * orders,) + a.shape[2:])
    if samples > 1:
        table_b, analysis_b = jnp.tile(table, (1, samples, 1, 1)), jnp.tile(analysis, (1, samples, 1, 1))
    else:
        table_b, analysis_b = table, analysis

    grads = degree_spectra(table_b, fold(grad_output), n_lat)
    spectra = degree_spectra(analysis_b, fold(saved_input), n_lat)
    grads_lm = grads.transpose(1, 0, 2)

    complex_width = mixing_weight.shape[1] // n_chan
    if n_chan == 2:
        sent = mix(grads_lm, mixing_weight, 1 - c, n_chan)
        arrived = lax.ppermute(sent, "chan", swap_pairs(2, 1))
        kept = mix(grads_lm, mixing_weight, c, n_chan)
        separate = (kept.astype(F32) + arrived.astype(F32)).astype(BF16)
    else:
        every = [mix(grads_lm, mixing_weight, jnp.int32(k), n_chan) for k in range(n_chan)]
        separate = lax.psum_scatter(jnp.stack(every), "chan", scatter_dimension=0, tiled=False)
    column = jnp.arange(width)
    place = (column % complex_width) * 2 + column // complex_width
    onehot = (place[:, None] == column[None, :]).astype(BF16)
    grad_spec_in = jnp.einsum("lmp,pq->mlq", separate, onehot, preferred_element_type=F32).astype(BF16)

    blocks = []
    out_halves = []
    total = samples * orders
    for h in range(HALVES):
        rows = slice(h * total // HALVES, (h + 1) * total // HALVES)
        blocks = jnp.stack(all_gather_line(grad_spec_in[rows], n_lat))
        out_halves.append(
            jnp.einsum(
                "kmlj,kmlq->mjq", analysis_b[:, rows], blocks, preferred_element_type=F32
            ).astype(BF16)
        )
    grad_input = jnp.concatenate(out_halves, axis=0).reshape(saved_input.shape)

    all_grads = [grads_lm]
    bit = n_dp // 2
    while bit:
        all_grads = all_grads + [lax.ppermute(a, "dp", swap_pairs(n_dp, bit)) for a in all_grads]
        bit //= 2
    order = [0]
    bit = n_dp // 2
    while bit:
        order = order + [o ^ bit for o in order]
        bit //= 2
    rows_dp = mixing_weight.shape[1] // n_dp
    if n_chan == 2 and n_dp % n_chan == 0:
        per = n_dp // n_chan
        inner = column % (2 * rows_dp)
        place = 2 * ((column // (2 * rows_dp)) * rows_dp + inner % rows_dp) + inner // rows_dp
        pick = (place[None, :] == column[:, None]).astype(BF16)
        apart = jnp.einsum("mlq,qp->lmp", spectra, pick, preferred_element_type=F32).astype(BF16)
        apart = apart.reshape(degrees, total, per, 2 * rows_dp).transpose(2, 0, 1, 3)
        other = lax.ppermute(apart, "chan", swap_pairs(2, 1))
        first = jnp.where(c == 0, apart, other)
        second = jnp.where(c == 0, other, apart)
        pieces = jnp.concatenate([first, second], axis=0)
    else:
        whole = lax.all_gather(spectra, "chan", axis=2, tiled=True)
        pieces = whole.reshape(total, degrees, n_dp, rows_dp, 2).transpose(2, 1, 0, 4, 3)
        pieces = pieces.reshape(n_dp, degrees, total, 2 * rows_dp)
    all_spectra = []
    for o in order:
        piece = lax.dynamic_index_in_dim(pieces, d ^ o, 0, keepdims=False)
        all_spectra.append(lax.ppermute(piece, "dp", swap_pairs(n_dp, o)) if o else piece)
    grad_weight = weight_gradient(all_grads, all_spectra, 1.0 / batch)
    return (grad_weight, grad_input)


def solution(mesh):
    in_specs = (
        P("dp", None, "lat", "chan"),
        P("dp", None, "lat", "chan"),
        P("lat", None, None),
        P(),
        P("lat", None, "chan"),
    )
    out_specs = (P("lat", "dp", "chan"), P("dp", None, "lat", "chan"))
    return jax.shard_map(
        on_device, mesh=mesh, in_specs=in_specs, out_specs=out_specs, check_vma=False
    )
```
